32 devices in a mesh: batch: 1 (over z), tmpl: 4 (over y), dap: 8 (over x, core).
Axes of the slice: x: 4, y: 4, z: 1, core: 2. Of those that a mesh axis runs over, the one named last changes fastest.
The devices are a block of a 4x4x8 slice.
Arguments:
- tmpl_act: bfloat16 [4, 512, 512, 64], P(('batch', 'tmpl'), 'dap')
- tmpl_mask: int32 [4], P('batch')
- pair_act: bfloat16 [512, 512, 128], P(('batch', 'dap'))
- pair_mask: int32 [512, 512], P(('batch', 'dap'))
- ln_tri: float32 [2, 2, 64], replicated
- w_ab: bfloat16 [2, 64, 4, 64], replicated
- b_ab: float32 [2, 4, 64], replicated
- w_gate: bfloat16 [2, 64, 64], replicated
- b_gate: float32 [2, 64], replicated
- ln_mix: float32 [2, 2, 64], replicated
- w_mix: bfloat16 [2, 64, 64], replicated
- b_mix: float32 [2, 64], replicated
- ln_tr: float32 [2, 2, 64], replicated
- w_up: bfloat16 [2, 64, 128], replicated
- b_up: float32 [2, 128], replicated
- w_down: bfloat16 [2, 128, 64], replicated
- b_down: float32 [2, 64], replicated
- ln_fin: float32 [2, 64], replicated
- w_query: bfloat16 [128, 4, 16], replicated
- w_key: bfloat16 [64, 4, 16], replicated
- w_value: bfloat16 [64, 4, 16], replicated
- w_out: bfloat16 [4, 16, 128], replicated
- b_out: float32 [128], replicated
Outputs:
- output: bfloat16 [512, 512, 128], P(('batch', 'dap'))
All inputs are finite; a program needn't handle non-finite values.
Results may differ from the reference program's by a relative error of at most 0.0158191.
Values are sent between devices in bfloat16 or wider.
A program may use at most 768 MiB of HBM per device.

```python
import jax
import jax.numpy as jnp
from jax import lax

NUM_TMPL = 4
RES_LEN = 512
C_TMPL = 64
C_MUL = 64
C_PAIR = 128
NUM_HEADS = 4
HEAD_DIM = 16
TRANS_MULT = 2
NUM_BLOCKS = 2
LN_EPS = 1e-5
MASK_BIAS = 1e9


def normal_draw(rng_key, arr_shape, std_scale):
    return std_scale * jax.random.normal(rng_key, arr_shape, jnp.float32)


def norm_params(rng_key, lead_shape, last_width):
    gain_key, bias_key = jax.random.split(rng_key)
    gain_vals = 1.0 + normal_draw(gain_key, lead_shape + (last_width,), 0.3)
    bias_vals = normal_draw(bias_key, lead_shape + (last_width,), 0.3)
    return jnp.stack([gain_vals, bias_vals], axis=-2)


def setup_inputs(seed: int = 0, part: int = 0) -> dict:
    base_key = jax.random.key(seed)
    part_keys = jax.random.split(jax.random.fold_in(base_key, part), 5)
    weight_keys = jax.random.split(base_key, 19)
    hidden_width = TRANS_MULT * C_TMPL
    mask_draw = jax.random.randint(part_keys[1], (NUM_TMPL,), 0, 2)
    forced_slot = jax.random.randint(part_keys[2], (), 0, NUM_TMPL)
    tmpl_mask = jnp.where((mask_draw > 0) | (jnp.arange(NUM_TMPL) == forced_slot), 1, 0).astype(jnp.int32)
    res_mask = jnp.where(jax.random.randint(part_keys[4], (RES_LEN,), 0, 3) > 0, 1, 0).astype(jnp.int32)
    pair_mask = res_mask[:, None] * res_mask[None, :]
    return {
        'tmpl_act': normal_draw(part_keys[0], (NUM_TMPL, RES_LEN, RES_LEN, C_TMPL), 1.0).astype(jnp.bfloat16),
        'tmpl_mask': tmpl_mask,
        'pair_act': normal_draw(part_keys[3], (RES_LEN, RES_LEN, C_PAIR), 1.0).astype(jnp.bfloat16),
        'pair_mask': pair_mask,
        'ln_tri': norm_params(weight_keys[0], (NUM_BLOCKS,), C_TMPL),
        'w_ab': normal_draw(weight_keys[1], (NUM_BLOCKS, C_TMPL, 4, C_MUL), C_TMPL ** -0.5).astype(jnp.bfloat16),
        'b_ab': normal_draw(weight_keys[2], (NUM_BLOCKS, 4, C_MUL), 1.0),
        'w_gate': normal_draw(weight_keys[3], (NUM_BLOCKS, C_TMPL, C_TMPL), C_TMPL ** -0.5).astype(jnp.bfloat16),
        'b_gate': normal_draw(weight_keys[4], (NUM_BLOCKS, C_TMPL), 1.0),
        'ln_mix': norm_params(weight_keys[5], (NUM_BLOCKS,), C_MUL),
        'w_mix': normal_draw(weight_keys[6], (NUM_BLOCKS, C_MUL, C_TMPL), C_MUL ** -0.5).astype(jnp.bfloat16),
        'b_mix': normal_draw(weight_keys[7], (NUM_BLOCKS, C_TMPL), 0.5),
        'ln_tr': norm_params(weight_keys[8], (NUM_BLOCKS,), C_TMPL),
        'w_up': normal_draw(weight_keys[9], (NUM_BLOCKS, C_TMPL, hidden_width), C_TMPL ** -0.5).astype(jnp.bfloat16),
        'b_up': normal_draw(weight_keys[10], (NUM_BLOCKS, hidden_width), 0.5),
        'w_down': normal_draw(weight_keys[11], (NUM_BLOCKS, hidden_width, C_TMPL), (0.5 * hidden_width) ** -0.5).astype(jnp.bfloat16),
        'b_down': normal_draw(weight_keys[12], (NUM_BLOCKS, C_TMPL), 0.5),
        'ln_fin': norm_params(weight_keys[13], (), C_TMPL),
        'w_query': normal_draw(weight_keys[14], (C_PAIR, NUM_HEADS, HEAD_DIM), C_PAIR ** -0.5).astype(jnp.bfloat16),
        'w_key': normal_draw(weight_keys[15], (C_TMPL, NUM_HEADS, HEAD_DIM), C_TMPL ** -0.5).astype(jnp.bfloat16),
        'w_value': normal_draw(weight_keys[16], (C_TMPL, NUM_HEADS, HEAD_DIM), C_TMPL ** -0.5).astype(jnp.bfloat16),
        'w_out': normal_draw(weight_keys[17], (NUM_HEADS, HEAD_DIM, C_PAIR), 2.0 * (NUM_HEADS * HEAD_DIM) ** -0.5).astype(jnp.bfloat16),
        'b_out': normal_draw(weight_keys[18], (C_PAIR,), 0.5),
    }


def layer_norm(values, gain_bias):
    val_f32 = values.astype(jnp.float32)
    row_mean = jnp.mean(val_f32, axis=-1, keepdims=True)
    centered = val_f32 - row_mean
    row_var = jnp.mean(centered * centered, axis=-1, keepdims=True)
    scaled = centered * lax.rsqrt(row_var + LN_EPS)
    return (scaled * gain_bias[0] + gain_bias[1]).astype(jnp.bfloat16)


def pair_block(tmpl_one, mask_f, block_w):
    ln_tri, w_ab, b_ab, w_gate, b_gate, ln_mix, w_mix, b_mix, ln_tr, w_up, b_up, w_down, b_down = block_w
    normed = layer_norm(tmpl_one, ln_tri)
    proj_all = jnp.dot(normed, w_ab.reshape(w_ab.shape[0], -1), preferred_element_type=jnp.float32)
    proj_all = proj_all.reshape(normed.shape[0], normed.shape[1], 4, -1) + b_ab
    left_act = (jax.nn.sigmoid(proj_all[:, :, 0]) * proj_all[:, :, 1] * mask_f).astype(jnp.bfloat16)
    right_act = (jax.nn.sigmoid(proj_all[:, :, 2]) * proj_all[:, :, 3] * mask_f).astype(jnp.bfloat16)
    mixed_sum = jnp.einsum('ikc,jkc->ijc', left_act.astype(jnp.float32), right_act.astype(jnp.float32))
    update = jnp.dot(layer_norm(mixed_sum, ln_mix), w_mix, preferred_element_type=jnp.float32) + b_mix
    gate_val = jax.nn.sigmoid(jnp.dot(normed, w_gate, preferred_element_type=jnp.float32) + b_gate)
    tmpl_one = (tmpl_one.astype(jnp.float32) + gate_val * update).astype(jnp.bfloat16)
    normed = layer_norm(tmpl_one, ln_tr)
    hidden = jax.nn.relu(jnp.dot(normed, w_up, preferred_element_type=jnp.float32) + b_up).astype(jnp.bfloat16)
    update = jnp.dot(hidden, w_down, preferred_element_type=jnp.float32) + b_down
    return (tmpl_one.astype(jnp.float32) + update).astype(jnp.bfloat16)


def template_stack(tmpl_one, mask_f, block_params, ln_fin):
    def block_step(carry_act, block_w):
        return pair_block(carry_act, mask_f, block_w), None
    stacked, unused_out = lax.scan(block_step, tmpl_one, block_params)
    return layer_norm(stacked, ln_fin)


def reference(tmpl_act, tmpl_mask, pair_act, pair_mask, ln_tri, w_ab, b_ab, w_gate, b_gate, ln_mix, w_mix, b_mix, ln_tr, w_up, b_up, w_down, b_down, ln_fin, w_query, w_key, w_value, w_out, b_out):
    mask_f = pair_mask.astype(jnp.float32)[:, :, None]
    block_params = (ln_tri, w_ab, b_ab, w_gate, b_gate, ln_mix, w_mix, b_mix, ln_tr, w_up, b_up, w_down, b_down)
    tmpl_fin = lax.map(lambda one_tmpl: template_stack(one_tmpl, mask_f, block_params, ln_fin), tmpl_act)
    by_row = jnp.swapaxes(tmpl_fin, 0, 1)
    bias_tmpl = MASK_BIAS * (tmpl_mask.astype(jnp.float32) - 1.0)
    head_width = NUM_HEADS * HEAD_DIM
    query_mat = w_query.reshape(C_PAIR, head_width)
    key_mat = w_key.reshape(C_TMPL, head_width)
    value_mat = w_value.reshape(C_TMPL, head_width)
    out_mat = w_out.reshape(head_width, C_PAIR)

    def row_attend(row_args):
        tmpl_row, pair_row = row_args
        query_row = jnp.dot(pair_row, query_mat, preferred_element_type=jnp.float32).astype(jnp.bfloat16).reshape(-1, NUM_HEADS, HEAD_DIM)
        key_row = jnp.dot(tmpl_row, key_mat, preferred_element_type=jnp.float32).astype(jnp.bfloat16).reshape(NUM_TMPL, -1, NUM_HEADS, HEAD_DIM)
        value_row = jnp.dot(tmpl_row, value_mat, preferred_element_type=jnp.float32).astype(jnp.bfloat16).reshape(NUM_TMPL, -1, NUM_HEADS, HEAD_DIM)
        logits = jnp.einsum('jhd,sjhd->jhs', query_row.astype(jnp.float32), key_row.astype(jnp.float32)) * HEAD_DIM ** -0.5 + bias_tmpl
        prob_row = jax.nn.softmax(logits, axis=-1).astype(jnp.bfloat16)
        attended = jnp.einsum('jhs,sjhd->jhd', prob_row.astype(jnp.float32), value_row.astype(jnp.float32)).astype(jnp.bfloat16)
        update = jnp.dot(attended.reshape(-1, head_width), out_mat, preferred_element_type=jnp.float32) + b_out
        return (pair_row.astype(jnp.float32) + update).astype(jnp.bfloat16)

    return lax.map(row_attend, (by_row, pair_act))
```

```python
import functools
import jax
import jax.numpy as jnp
from jax import lax
from jax.experimental import pallas as pl
from jax.experimental.pallas import tpu as pltpu
from jax.sharding import PartitionSpec as P

LN_EPS = 1e-5
MASK_BIAS = 1e9
BLOCK_ARGS = 13
F32, BF16 = jnp.float32, jnp.bfloat16
NQ = 2
IB = 16
GB = 8
CB = 8
LANES = 128
PAIR_GROUP = 4
HEAD_GROUP = 4
CORES = 2


def dot(lhs, rhs, lhs_dim=1, rhs_dim=0):
    return lax.dot_general(lhs, rhs, (((lhs_dim,), (rhs_dim,)), ((), ())), preferred_element_type=F32)


def wide(param, width):
    return jnp.concatenate([param] * (width // LANES), axis=-1)


def norm_lead(val, gain, bias):
    width = val.shape[-1]
    mean = jnp.mean(val, axis=0, keepdims=True)
    cen = val - mean
    var = jnp.mean(cen * cen, axis=0, keepdims=True)
    return (cen * lax.rsqrt(var + LN_EPS) * wide(gain, width) + wide(bias, width)).astype(BF16)


def project(normed, w_ab, b_ab, mask_row):
    proj = dot(w_ab, normed) + wide(b_ab, normed.shape[-1])
    ch = proj.shape[0] // 4
    left = (jnp.tanh(proj[:ch]) + 1.0) * proj[ch:2 * ch] * mask_row
    right = (jnp.tanh(proj[2 * ch:3 * ch]) + 1.0) * proj[3 * ch:] * mask_row
    return left, right


def put_row(scr, row, rows, block, val):
    for lb in range(val.shape[1] // LANES):
        scr[block + lb, pl.ds(row, val.shape[0], stride=rows), :] = val[:, lb * LANES:(lb + 1) * LANES]


def flush(scr, out_ref):
    ch, rows, width = out_ref.shape
    for lb in range(width // LANES):
        out_ref[:, :, lb * LANES:(lb + 1) * LANES] = scr[lb].reshape(ch, rows, LANES).astype(BF16)


def head_kernel(t_ref, mask_ref, perm_ref, par_ref, wab_ref, *refs):
    a_ref, b_ref, u_ref, tt_ref, a_scr, b_scr = refs[-6:]
    rows, ch, cols = t_ref.shape
    wid = cols // NQ
    off_ln, off_ab = 0, 2 * ch
    ordered = dot(t_ref[...].reshape(rows * ch, cols), perm_ref[...])
    tt_ref[...] = ordered.astype(BF16).reshape(rows, ch, cols)
    for q in range(NQ):
        lane = slice(q * wid, (q + 1) * wid)
        for g in range(0, rows, HEAD_GROUP):
            rng = range(g, g + HEAD_GROUP)
            val = jnp.concatenate([tt_ref[r, :, lane] for r in rng], axis=1).astype(F32)
            normed = norm_lead(val, par_ref[off_ln:off_ln + ch], par_ref[off_ln + ch:off_ln + 2 * ch])
            mask_all = jnp.concatenate([mask_ref[r:r + 1, lane] for r in rng], axis=1)
            left, right = project(normed, wab_ref[...], par_ref[off_ab:off_ab + 4 * ch], mask_all)
            for n, r in enumerate(rng):
                part = slice(n * wid, (n + 1) * wid)
                u_ref[r, :, lane] = normed[:, part]
                put_row(a_scr, r, rows, q * wid // LANES, left[:, part])
                put_row(b_scr, r, rows, q * wid // LANES, right[:, part])
    flush(a_scr, a_ref)
    flush(b_scr, b_ref)


def pair_kernel(steps, na, sources, last, order_ref, *refs):
    refs = list(refs)
    a_refs, refs = refs[:na], refs[na:]
    b_refs = []
    for count in sources:
        b_refs.append(refs[:count])
        refs = refs[count:]
    t_ref, u_ref, mask_ref, lnx_ref, wmix_ref, wgate_ref, wup_ref, wdown_ref, par_ref = refs[:9]
    refs = refs[9:]
    if last:
        out_ref, x_scr = refs[:2]
        g_scrs = refs[2:]
    else:
        wab_ref, t_out, u_out, a_out = refs[:4]
        g_scrs = refs[-len(sources):]
        x_scr, a_scr, b_scr = refs[-len(sources) - 3:-len(sources)]
        b_outs = refs[4:-len(sources) - 3]
    step = pl.program_id(0)
    ch = t_ref.shape[1]
    rows, wid = IB, t_ref.shape[2]

    @pl.when(step < steps)
    def _():
        for c in range(CB):
            for g_scr, part in zip(g_scrs, b_refs):
                sub = part[0].shape[1]
                for n, b_ref in enumerate(part):
                    g_scr[c, pl.ds(pl.multiple_of(order_ref[n] * sub, sub), sub), :] = b_ref[c]
            acc = None
            for a_ref, g_scr in zip(a_refs, g_scrs):
                term = dot(a_ref[c], g_scr[c], 1, 1)
                acc = term if acc is None else acc + term
            x_scr[step * CB + c] = acc

    @pl.when(step >= steps)
    def _():
        base = (step - steps) * rows
        par = lambda n, size=1: par_ref[n * ch:(n + size) * ch, :]
        for g in range(rows // GB):
            val = x_scr[:, pl.ds(pl.multiple_of(base + g * GB, GB), GB), :]
            mixed = norm_lead(val, lnx_ref[0], lnx_ref[1]).reshape(ch * GB, wid)
            upd8 = dot(wmix_ref[...], mixed).reshape(GB, ch, wid)
            for h in range(0, GB, PAIR_GROUP):
                rng = range(g * GB + h, g * GB + h + PAIR_GROUP)
                u_all = jnp.concatenate([u_ref[r] for r in rng], axis=1)
                t_all = jnp.concatenate([t_ref[r] for r in rng], axis=1).astype(F32)
                upd = jnp.concatenate([upd8[h + n] for n in range(PAIR_GROUP)], axis=1)
                full = PAIR_GROUP * wid
                gate = jnp.tanh(dot(wgate_ref[...], u_all) + wide(par(0), full)) + 1.0
                t_all = (t_all + gate * (upd + wide(par(1), full))).astype(BF16)
                normed = norm_lead(t_all.astype(F32), par(3), par(4))
                hidden = jnp.maximum(dot(wup_ref[...], normed) + wide(par(7, 2), full), 0.0).astype(BF16)
                upd = dot(wdown_ref[...], hidden) + wide(par(2), full)
                t_all = (t_all.astype(F32) + upd).astype(BF16)
                normed = norm_lead(t_all.astype(F32), par(5), par(6))
                if last:
                    for n, r in enumerate(rng):
                        out_ref[r] = normed[:, n * wid:(n + 1) * wid]
                else:
                    mask_all = jnp.concatenate([mask_ref[r:r + 1, :] for r in rng], axis=1)
                    left, right = project(normed, wab_ref[...], par(9, 4), mask_all)
                    for n, r in enumerate(rng):
                        cols = slice(n * wid, (n + 1) * wid)
                        t_out[r] = t_all[:, cols]
                        u_out[r] = normed[:, cols]
                        put_row(a_scr, r, rows, 0, left[:, cols])
                        put_row(b_scr, r, rows, 0, right[:, cols])
        if not last:
            flush(a_scr, a_out)
            if len(b_outs) == 1:
                flush(b_scr, b_outs[0])
            else:
                per = pl.num_programs(0) - steps
                for n, b_out in enumerate(b_outs):
                    here = (step - steps) // (per // len(b_outs)) == n
                    pl.when(here)(functools.partial(flush, b_scr, b_out))


def attend_kernel(heads, bias_ref, t_ref, z_ref, wq_ref, wkv_ref, o_ref):
    num, rows, _, wid = t_ref.shape
    dim = wq_ref.shape[0] // heads

    def one_row(row, carry):
        zed = z_ref[row].reshape(wid, -1)
        query = dot(wq_ref[...], zed, 1, 1).astype(BF16).astype(F32)
        logits, values = [], []
        for s in range(num):
            kv = dot(wkv_ref[...], t_ref[s, row]).astype(BF16).astype(F32)
            half = kv.shape[0] // 2
            values.append(kv[half:].reshape(heads, dim, wid))
            score = jnp.sum((query * kv[:half]).reshape(heads, dim, wid), axis=1, keepdims=True)
            logits.append(score * dim ** -0.5 + bias_ref[s])
        top = functools.reduce(jnp.maximum, logits)
        exps = [jnp.exp(lg - top) for lg in logits]
        total = functools.reduce(jnp.add, exps)
        out = None
        for s in range(num):
            term = (exps[s] / total).astype(BF16).astype(F32) * values[s]
            out = term if out is None else out + term
        o_ref[row] = out.reshape(heads * dim, wid).astype(BF16)
        return carry

    lax.fori_loop(0, rows, one_row, 0)


def out_kernel(num, per_part, _, *refs):
    o_refs, (z_ref, w_ref, b_ref) = refs[:num], refs[num:num + 3]
    y_ref = refs[-1]
    rows, dap, sub, width = z_ref.shape
    for n, o_ref in enumerate(o_refs):
        @pl.when(pl.program_id(0) // per_part == n)
        def _(o_ref=o_ref):
            for row in range(rows):
                upd = dot(o_ref[row], w_ref[...], 0, 0) + b_ref[...]
                y_ref[row] = (z_ref[row].astype(F32) + upd.reshape(dap, sub, width)).astype(BF16)


def whole(arr):
    return pl.BlockSpec(arr.shape, lambda *_: (0,) * arr.ndim)


def sds(shape, dtype=BF16):
    return jax.ShapeDtypeStruct(shape, dtype)


def cost(flops, nbytes):
    return pl.CostEstimate(flops=flops, bytes_accessed=nbytes, transcendentals=0)


def col(param):
    return jnp.broadcast_to(param[..., None], param.shape + (LANES,))


def head(t_nat, mask_f, part, perm, par, w_ab, into, after):
    rows, ch, cols = t_nat.shape
    mine = rows // NQ
    first = part * (mine // IB)
    row_block = pl.BlockSpec((IB, ch, cols), lambda s: (first + s, 0, 0))
    extra = list(into) + list(after)
    return pl.pallas_call(
        head_kernel,
        grid=(mine // IB,),
        in_specs=[row_block, pl.BlockSpec((IB, cols), lambda s: (first + s, 0)),
                  whole(perm), whole(par), whole(w_ab)] + [pl.BlockSpec(memory_space=pl.ANY)] * len(extra),
        out_specs=[pl.BlockSpec((ch, IB, cols), lambda s: (0, first + s, 0)),
                   pl.BlockSpec((ch, IB, cols), lambda s: (0, s, 0)), row_block, row_block],
        out_shape=[sds((ch, rows, cols)), sds((ch, mine, cols)), sds((rows, ch, cols)), sds((rows, ch, cols))],
        input_output_aliases={5: 0, 6: 2, 7: 3} if into else {},
        scratch_shapes=[pltpu.VMEM((cols // LANES, ch * IB, LANES), F32)] * 2,
        cost_estimate=cost(2 * mine * cols * ch * 16 * ch, 5 * mine * cols * ch * 2),
    )(t_nat, mask_f, perm, par, w_ab, *extra)


def pair(q, order, a_parts, b_parts, b_index, t_arr, u_arr, mask_f, weights, next_w, split_b, last):
    ch = a_parts[0].shape[0]
    rows, cols = mask_f.shape
    wid = cols // NQ
    dap = len(b_parts[0])
    sub = wid // dap
    steps, row_steps = ch // CB, rows // IB
    tri = lambda s: jnp.minimum(s, steps - 1)
    row = lambda s: jnp.maximum(s - steps, 0)
    fixed = lambda arr: pl.BlockSpec(arr.shape, lambda s, o: (0,) * arr.ndim)
    in_specs = [pl.BlockSpec((CB,) + a.shape[1:], lambda s, o: (tri(s), 0, 0)) for a in a_parts]
    scratch_b = []
    for part, where in zip(b_parts, b_index):
        depth = part[0].shape[2]
        in_specs += [pl.BlockSpec((CB, sub, depth), lambda s, o, where=where: (tri(s), where, 0))] * dap
        scratch_b.append(pltpu.VMEM((CB, wid, depth), BF16))
    t_col = 0 if t_arr.shape[2] == wid else q
    in_specs += [pl.BlockSpec((IB, ch, wid), lambda s, o: (row(s), 0, t_col))] * 2
    in_specs += [pl.BlockSpec((IB, wid), lambda s, o: (row(s), q))]
    tail = list(weights) + list(next_w)
    in_specs += [fixed(w) for w in tail]
    scratch = [pltpu.VMEM((ch, rows, wid), F32)]
    row_out = pl.BlockSpec((IB, ch, wid), lambda s, o: (row(s), 0, 0))
    if last:
        out_shape, out_specs = [sds((rows, ch, wid))], [row_out]
    else:
        out_shape = [sds((rows, ch, wid))] * 2 + [sds((ch, rows, wid))]
        out_specs = [row_out] * 2 + [pl.BlockSpec((ch, IB, wid), lambda s, o: (0, row(s), 0))]
        per = row_steps // split_b
        for n in range(split_b):
            out_shape.append(sds((ch, rows // split_b, wid)))
            out_specs.append(pl.BlockSpec((ch, IB, wid), lambda s, o, n=n: (0, jnp.clip(row(s) - n * per, 0, per - 1), 0)))
        scratch += [pltpu.VMEM((wid // LANES, ch * IB, LANES), F32)] * 2
    flops = 2 * rows * wid * ch * (cols + 40 * ch)
    return pl.pallas_call(
        functools.partial(pair_kernel, steps, len(a_parts), [dap] * len(b_parts), last),
        grid_spec=pltpu.PrefetchScalarGridSpec(
            num_scalar_prefetch=1, grid=(steps + row_steps,), in_specs=in_specs, out_specs=out_specs,
            scratch_shapes=scratch + scratch_b),
        out_shape=out_shape,
        cost_estimate=cost(flops, 4 * rows * cols * ch),
    )(order, *a_parts, *sum(b_parts, []), t_arr, u_arr, mask_f, *tail)


def attend(q, t_all, pair_loc, bias, w_q, w_kv, heads, quarter):
    num, rows, ch, wid = t_all.shape
    _, dap, per, width = pair_loc.shape
    ib = 8
    grid_spec = pltpu.PrefetchScalarGridSpec(
        num_scalar_prefetch=1,
        grid=(rows // ib,),
        in_specs=[pl.BlockSpec(memory_space=pltpu.SMEM),
                  pl.BlockSpec((num, ib, ch, wid), lambda s, r: (0, s, 0, 0)),
                  pl.BlockSpec((ib, dap, per // NQ, width), lambda s, r: (r[0] * (rows // ib) + s, 0, q, 0)),
                  pl.BlockSpec(w_q.shape, lambda s, r: (0, 0)),
                  pl.BlockSpec(w_kv.shape, lambda s, r: (0, 0))],
        out_specs=pl.BlockSpec((ib, w_q.shape[0], wid), lambda s, r: (s, 0, 0)),
    )
    return pl.pallas_call(
        lambda r_ref, *refs: attend_kernel(heads, *refs),
        grid_spec=grid_spec,
        out_shape=sds((rows, w_q.shape[0], wid)),
        cost_estimate=cost(2 * rows * wid * (num * ch * 4 * ch + width * ch), 8 * rows * wid * ch),
    )(quarter, bias, t_all, pair_loc, w_q, w_kv)


def project_out(q, where, o_parts, pair_loc, w_out, b_out, into):
    rows, dap, per, width = pair_loc.shape
    num = len(o_parts)
    ib = 8
    per_part = rows // num // ib
    z_spec = pl.BlockSpec((ib, dap, per // NQ, width), lambda s, w: (w[s // per_part] * per_part + s % per_part, 0, q, 0))
    o_specs = [pl.BlockSpec((ib,) + o.shape[1:], lambda s, w, n=n: (jnp.clip(s - n * per_part, 0, per_part - 1), 0, 0))
               for n, o in enumerate(o_parts)]
    fixed = lambda arr: pl.BlockSpec(arr.shape, lambda s, w: (0, 0))
    extra = [] if into is None else [into]
    return pl.pallas_call(
        functools.partial(out_kernel, num, per_part),
        grid_spec=pltpu.PrefetchScalarGridSpec(
            num_scalar_prefetch=1, grid=(rows // ib,),
            in_specs=o_specs + [z_spec, fixed(w_out), fixed(b_out)] + [pl.BlockSpec(memory_space=pl.ANY)] * len(extra),
            out_specs=z_spec),
        out_shape=sds(pair_loc.shape),
        input_output_aliases={} if into is None else {num + 4: 0},
        cost_estimate=cost(4 * rows * dap * per * width * o_parts[0].shape[1] // NQ, 6 * rows * dap * per * width // NQ),
    )(where, *o_parts, pair_loc, w_out, b_out, *extra)


def mix_weights(blk):
    ln_mix, w_mix = blk[5:7]
    ch = w_mix.shape[0]
    lnx = jnp.broadcast_to(ln_mix[:, :, None, None], (2, ch, GB, LANES))
    eye = jnp.eye(GB, dtype=BF16)
    return lnx, ((w_mix.T * 0.5)[None, :, :, None] * eye[:, None, None, :]).reshape(GB * ch, ch * GB)


def block_weights(blk, par):
    w_gate, w_up, w_down = blk[3], blk[9], blk[11]
    return mix_weights(blk) + (w_gate.T * 0.5, w_up.T, w_down.T, par)


def columns(blk, fin, next_b):
    _, _, _, _, b_gate, _, _, b_mix, ln_tr, _, b_up, _, b_down = blk
    return [b_gate * 0.5, b_mix * 0.5, b_down, *ln_tr, *fin, b_up] + ([] if next_b is None else [next_b.reshape(-1) * 0.5])


def half_w_ab(w_ab):
    return w_ab.reshape(w_ab.shape[0], -1).T * 0.5


def ring_step(val, axis, size, step, cores, flip=False):
    pairs = []
    for src in range(size * cores):
        chip, core = src // cores, src % cores
        pairs.append((src, (chip + step) % size * cores + (cores - 1 - core if flip else core)))
    return lax.ppermute(val, axis, pairs)


def ring_gather(val, axis, size, cores, forward):
    back = ring_step(val, axis, size, 1, cores)
    on = ring_step(val, axis, size, -1, cores)
    far = ring_step(back if forward > 0 else on, axis, size, forward, cores)
    return [val, back, on, far]


def solution(mesh):
    tmpl_spec = P(('batch', 'tmpl'), 'dap')
    row_spec = P(('batch', 'dap'))
    dap, tmpl = mesh.shape['dap'], mesh.shape['tmpl']
    chips = dap // CORES

    def gather(part, forward):
        mine = ring_gather(part, 'dap', chips, CORES, forward)
        other = [ring_step(val, 'dap', chips, 0, CORES, True) for val in mine]
        return mine + other

    def local_fn(tmpl_loc, tmpl_mask, pair_loc, mask_loc, *weights):
        _, rows, cols, ch = tmpl_loc.shape
        blk0, blk1 = (tuple(w[i] for w in weights[:BLOCK_ARGS]) for i in range(2))
        ln_fin, w_query, w_key, w_value, w_out, b_out = weights[BLOCK_ARGS:]
        heads = w_query.shape[1]
        per = cols // dap
        sub = per // NQ
        me = lax.axis_index('dap').astype(jnp.int32)
        chip, core = me // CORES, me % CORES
        hops = jnp.array([0, -1, 1, 2], jnp.int32)
        near = (chip + hops) % chips * CORES
        order = jnp.concatenate([near + core, near + (CORES - 1 - core)])

        lane = jnp.arange(cols, dtype=jnp.int32)
        source = lane // sub % dap * per + lane // (dap * sub) * sub + lane % sub
        perm = (lane[:, None] == source[None, :]).astype(BF16)
        mask_f = mask_loc.astype(F32).reshape(rows, dap, NQ, sub).swapaxes(1, 2).reshape(rows, cols)
        t_nat = tmpl_loc.reshape(rows, cols, ch).swapaxes(1, 2)
        head_par = [*blk0[0], blk0[2].reshape(-1) * 0.5]
        pars = [head_par, columns(blk0, blk1[0], blk1[2]), columns(blk1, ln_fin, None)]
        par_head = col(jnp.concatenate(pars[0]))
        par0, par1 = col(jnp.concatenate(pars[1])), col(jnp.concatenate(pars[2]))

        first_w, next_w = block_weights(blk0, par0), (half_w_ab(blk1[1]),)
        second_w = block_weights(blk1, par1)
        w_q = w_query.reshape(w_query.shape[0], -1).T
        w_kv = jnp.concatenate([w_key.reshape(ch, -1), w_value.reshape(ch, -1)], axis=1).T

        b1, into, after = [], (), ()
        for part in range(NQ):
            a1, b, u1, t1 = head(t_nat, mask_f, part, perm, par_head, half_w_ab(blk0[1]), into, after)
            into, after = (a1, u1, t1), first_w + next_w + second_w + (w_q, w_kv)
            b1.append(gather(b, 1 if part == 0 else -1))

        t2, u2, a2, b2 = [], [], [], []
        for q in range(NQ):
            split = 1 if q < NQ - 1 else NQ
            out = pair(q, order, [a1], [b1[q]], [0], t1, u1, mask_f, first_w, next_w, split, False)
            t2.append(out[0])
            u2.append(out[1])
            a2.append(out[2])
            b2.append([gather(b, 1 if q < NQ - 1 else -1) for b in out[3:]])

        bias = MASK_BIAS * (tmpl_mask.astype(F32) - 1.0)
        z_view = pair_loc.reshape(rows, dap, per, pair_loc.shape[2])
        quarter = lax.axis_index('tmpl').astype(jnp.int32).reshape(1)
        where = (quarter + hops) % tmpl
        z_out = None
        for q in range(NQ):
            b_parts = [b2[k][0] for k in range(NQ - 1)] + [b2[NQ - 1][q]]
            fin, = pair(q, order, a2, b_parts, [q] * (NQ - 1) + [0], t2[q], u2[q], mask_f, second_w, (), 0, True)
            fin = fin.reshape(tmpl, rows // tmpl, ch, fin.shape[2])
            t_all = lax.all_to_all(fin, 'tmpl', 0, 0)
            o_loc = attend(q, t_all, z_view, bias, w_q, w_kv, heads, quarter)
            o_parts = ring_gather(o_loc, 'tmpl', tmpl, 1, 1 if q == 0 else -1)
            z_out = project_out(q, where, o_parts, z_view, w_out.reshape(-1, w_out.shape[2]), b_out[None], z_out)
        return z_out.reshape(pair_loc.shape)

    in_specs = (tmpl_spec, P('batch'), row_spec, row_spec) + (P(),) * (BLOCK_ARGS + 6)
    return jax.shard_map(local_fn, mesh=mesh, in_specs=in_specs, out_specs=row_spec, check_vma=False)
```

```python
import functools
import math
import jax
import jax.numpy as jnp
from jax import lax
from jax.experimental import pallas as pl
from jax.experimental.pallas import tpu as pltpu
from jax.sharding import PartitionSpec as P

LN_EPS = 1e-5
MASK_BIAS = 1e9
BLOCK_ARGS = 13
F32, BF16 = jnp.float32, jnp.bfloat16
UNIT = 16
NQ = 2
PIECES = (2, 2)
IB = 16
GB = 8
CB = 16
LANES = 128
OUT_VMEM = 20 << 20
VMEM_LIMIT = 40 << 20
HEAD_GROUP = 4
CORES = 2


def dot(lhs, rhs, lhs_dim=1, rhs_dim=0):
    return lax.dot_general(lhs, rhs, (((lhs_dim,), (rhs_dim,)), ((), ())), preferred_element_type=F32)


def wide(param, width):
    return jnp.concatenate([param] * (width // LANES), axis=-1)


def norm_lead(val, gain, bias):
    width = val.shape[-1]
    mean = jnp.mean(val, axis=0, keepdims=True)
    cen = val - mean
    var = jnp.mean(cen * cen, axis=0, keepdims=True)
    return (cen * lax.rsqrt(var + LN_EPS) * wide(gain, width) + wide(bias, width)).astype(BF16)


def project(normed, w_ab, b_ab, mask_row):
    proj = dot(w_ab, normed) + wide(b_ab, normed.shape[-1])
    ch = proj.shape[0] // 4
    left = (jnp.tanh(proj[:ch]) + 1.0) * proj[ch:2 * ch] * mask_row
    right = (jnp.tanh(proj[2 * ch:3 * ch]) + 1.0) * proj[3 * ch:] * mask_row
    return left, right


def put_row(scr, row, rows, block, val):
    for lb in range(val.shape[1] // LANES):
        scr[block + lb, pl.ds(row, val.shape[0], stride=rows), :] = val[:, lb * LANES:(lb + 1) * LANES]


def flush(scr, out_ref):
    ch, rows, width = out_ref.shape
    for lb in range(width // LANES):
        out_ref[:, :, lb * LANES:(lb + 1) * LANES] = scr[lb].reshape(ch, rows, LANES).astype(BF16)


def head_kernel(t_ref, mask_ref, perm_ref, par_ref, wab_ref, *refs):
    a_ref, b_ref, u_ref, tt_ref, a_scr, b_scr = refs[-6:]
    rows, ch, cols = t_ref.shape
    wid = cols // NQ
    off_ln, off_ab = 0, 2 * ch
    ordered = dot(t_ref[...].reshape(rows * ch, cols), perm_ref[...])
    tt_ref[...] = ordered.astype(BF16).reshape(rows, ch, cols)
    for q in range(NQ):
        lane = slice(q * wid, (q + 1) * wid)
        for g in range(0, rows, HEAD_GROUP):
            rng = range(g, g + HEAD_GROUP)
            val = jnp.concatenate([tt_ref[r, :, lane] for r in rng], axis=1).astype(F32)
            normed = norm_lead(val, par_ref[off_ln:off_ln + ch], par_ref[off_ln + ch:off_ln + 2 * ch])
            mask_all = jnp.concatenate([mask_ref[r:r + 1, lane] for r in rng], axis=1)
            left, right = project(normed, wab_ref[...], par_ref[off_ab:off_ab + 4 * ch], mask_all)
            for n, r in enumerate(rng):
                part = slice(n * wid, (n + 1) * wid)
                u_ref[r, :, lane] = normed[:, part]
                put_row(a_scr, r, rows, q * wid // LANES, left[:, part])
                put_row(b_scr, r, rows, q * wid // LANES, right[:, part])
    flush(a_scr, a_ref)
    flush(b_scr, b_ref)


def pair_kernel(steps, na, sources, split, order_ref, *refs):
    refs = list(refs)
    a_refs, refs = refs[:na], refs[na:]
    last = not split
    b_refs = []
    for count in sources:
        b_refs.append(refs[:count])
        refs = refs[count:]
    t_ref, u_ref, mask_ref, lnx_ref, wmix_ref, wgate_ref, wup_ref, wdown_ref, par_ref = refs[:9]
    refs = refs[9:]
    if last:
        out_ref, x_scr = refs[:2]
        g_scrs = refs[2:]
    else:
        wab_ref, t_out, u_out, a_out = refs[:4]
        g_scrs = refs[-len(sources):]
        x_scr, a_scr, b_scr = refs[-len(sources) - 3:-len(sources)]
        b_outs = refs[4:-len(sources) - 3]
    step = pl.program_id(0)
    ch = t_ref.shape[1]
    rows, wid = IB, t_ref.shape[2]

    @pl.when(step < steps)
    def _():
        for c in range(CB):
            for g_scr, part in zip(g_scrs, b_refs):
                unit = len(part) * UNIT
                for n, b_ref in enumerate(part):
                    for k in range(b_ref.shape[1] // UNIT):
                        where = pl.ds(pl.multiple_of(k * unit + order_ref[n] * UNIT, UNIT), UNIT)
                        g_scr[c, where, :] = b_ref[c, k * UNIT:(k + 1) * UNIT, :]
            acc = None
            for a_ref, g_scr in zip(a_refs, g_scrs):
                term = dot(a_ref[c], g_scr[c], 1, 1)
                acc = term if acc is None else acc + term
            x_scr[step * CB + c] = acc

    @pl.when(step >= steps)
    def _():
        base = (step - steps) * rows
        par = lambda n, size=1: par_ref[n * ch:(n + size) * ch, :]

        def group(g, carry):
            at = pl.multiple_of(g * GB, GB)
            val = x_scr[:, pl.ds(pl.multiple_of(base + at, GB), GB), :]
            mixed = norm_lead(val, lnx_ref[0], lnx_ref[1]).reshape(ch * GB, wid)
            upd = dot(wmix_ref[...], mixed).reshape(GB, ch, wid)
            side_by_side = lambda val: jnp.concatenate([val[n] for n in range(GB)], axis=1)
            full = GB * wid
            gate = jnp.tanh(dot(wgate_ref[...], side_by_side(u_ref[pl.ds(at, GB)])) + wide(par(0), full)) + 1.0
            t_all = side_by_side(t_ref[pl.ds(at, GB)]).astype(F32)
            t_all = (t_all + gate * (side_by_side(upd) + wide(par(1), full))).astype(BF16)
            normed = norm_lead(t_all.astype(F32), par(3), par(4))
            hidden = jnp.maximum(dot(wup_ref[...], normed) + wide(par(7, 2), full), 0.0).astype(BF16)
            upd = dot(wdown_ref[...], hidden) + wide(par(2), full)
            t_all = (t_all.astype(F32) + upd).astype(BF16)
            normed = norm_lead(t_all.astype(F32), par(5), par(6))
            if not last:
                masks = mask_ref[pl.ds(at, GB), :]
                left, right = project(normed, wab_ref[...], par(9, 4), jnp.concatenate([masks[n:n + 1] for n in range(GB)], axis=1))
            for n in range(GB):
                cols = slice(n * wid, (n + 1) * wid)
                if last:
                    out_ref[at + n] = normed[:, cols]
                else:
                    t_out[at + n] = t_all[:, cols]
                    u_out[at + n] = normed[:, cols]
                    put_row(a_scr, at + n, rows, 0, left[:, cols])
                    put_row(b_scr, at + n, rows, 0, right[:, cols])
            return carry

        lax.fori_loop(0, rows // GB, group, 0, unroll=last)
        if not last:
            flush(a_scr, a_out)
            for b_out, (first, count) in zip(b_outs, split):
                here = (step >= steps + first) & (step < steps + first + count)
                pl.when(here)(functools.partial(flush, b_scr, b_out))


def attend_kernel(heads, bias_ref, t_ref, z_ref, wq_ref, wkv_ref, o_ref):
    num, rows, _, wid = t_ref.shape
    dim = wq_ref.shape[0] // heads

    def one_row(row, carry):
        zed = jnp.concatenate([z_ref[row, :, k:k + UNIT, :] for k in range(0, z_ref.shape[2], UNIT)]).reshape(wid, -1)
        query = dot(wq_ref[...], zed, 1, 1).astype(BF16).astype(F32)
        logits, values = [], []
        for s in range(num):
            kv = dot(wkv_ref[...], t_ref[s, row]).astype(BF16).astype(F32)
            half = kv.shape[0] // 2
            values.append(kv[half:].reshape(heads, dim, wid))
            score = jnp.sum((query * kv[:half]).reshape(heads, dim, wid), axis=1, keepdims=True)
            logits.append(score * dim ** -0.5 + bias_ref[s])
        top = functools.reduce(jnp.maximum, logits)
        exps = [jnp.exp(lg - top) for lg in logits]
        total = functools.reduce(jnp.add, exps)
        out = None
        for s in range(num):
            term = (exps[s] / total).astype(BF16).astype(F32) * values[s]
            out = term if out is None else out + term
        o_ref[row] = out.reshape(heads * dim, wid).astype(BF16)
        return carry

    lax.fori_loop(0, rows, one_row, 0, unroll=rows)


def out_kernel(num, per_part, _, *refs):
    o_refs, (z_ref, w_ref, b_ref) = refs[:num], refs[num:num + 3]
    y_ref = refs[-1]
    rows, dap, sub, width = z_ref.shape
    for n, o_ref in enumerate(o_refs):
        @pl.when(pl.program_id(0) // per_part == n)
        def _(o_ref=o_ref):
            def one_row(row, carry):
                upd = (dot(o_ref[row], w_ref[...], 0, 0) + b_ref[...]).reshape(sub // UNIT, dap, UNIT, width)
                for k in range(sub // UNIT):
                    part = slice(k * UNIT, (k + 1) * UNIT)
                    y_ref[row, :, part, :] = (z_ref[row, :, part, :].astype(F32) + upd[k]).astype(BF16)
                return carry

            lax.fori_loop(0, rows, one_row, 0, unroll=4)


def whole(arr):
    return pl.BlockSpec(arr.shape, lambda *_: (0,) * arr.ndim)


def sds(shape, dtype=BF16):
    return jax.ShapeDtypeStruct(shape, dtype)


def cost(flops, nbytes):
    return pl.CostEstimate(flops=flops, bytes_accessed=nbytes, transcendentals=0)


def col(param):
    return jnp.broadcast_to(param[..., None], param.shape + (LANES,))


def head(t_nat, mask_f, part, perm, par, w_ab, into, after):
    rows, ch, cols = t_nat.shape
    mine = rows // NQ
    first = part * (mine // IB)
    row_block = pl.BlockSpec((IB, ch, cols), lambda s: (first + s, 0, 0))
    extra = list(into) + list(after)
    return pl.pallas_call(
        head_kernel,
        grid=(mine // IB,),
        in_specs=[row_block, pl.BlockSpec((IB, cols), lambda s: (first + s, 0)),
                  whole(perm), whole(par), whole(w_ab)] + [pl.BlockSpec(memory_space=pl.ANY)] * len(extra),
        out_specs=[pl.BlockSpec((ch, IB, cols), lambda s: (0, first + s, 0)),
                   pl.BlockSpec((ch, IB, cols), lambda s: (0, s, 0)), row_block, row_block],
        out_shape=[sds((ch, rows, cols)), sds((ch, mine, cols)), sds((rows, ch, cols)), sds((rows, ch, cols))],
        input_output_aliases={5: 0, 6: 2, 7: 3} if into else {},
        scratch_shapes=[pltpu.VMEM((cols // LANES, ch * IB, LANES), F32)] * 2,
        cost_estimate=cost(2 * mine * cols * ch * 16 * ch, 5 * mine * cols * ch * 2),
    )(t_nat, mask_f, perm, par, w_ab, *extra)


def pair(where, wid, order, a_parts, b_parts, b_index, t_arr, u_arr, t_index, mask_f, weights, next_w, split):
    ch = a_parts[0].shape[0]
    rows, cols = mask_f.shape
    dap = len(b_parts[0])
    sub = wid // dap
    steps, row_steps = ch // CB, rows // IB
    tri = lambda s: jnp.minimum(s, steps - 1)
    row = lambda s: jnp.maximum(s - steps, 0)
    fixed = lambda arr: pl.BlockSpec(arr.shape, lambda s, o: (0,) * arr.ndim)
    in_specs = [pl.BlockSpec((CB,) + a.shape[1:], lambda s, o: (tri(s), 0, 0)) for a in a_parts]
    scratch_b = []
    for part, at in zip(b_parts, b_index):
        depth = part[0].shape[2]
        in_specs += [pl.BlockSpec((CB, sub, depth), lambda s, o, at=at: (tri(s), at, 0))] * dap
        scratch_b.append(pltpu.VMEM((CB, wid, depth), BF16))
    in_specs += [pl.BlockSpec((IB, ch, wid), lambda s, o: (row(s), 0, t_index))] * 2
    in_specs += [pl.BlockSpec((IB, wid), lambda s, o: (row(s), where))]
    tail = list(weights) + list(next_w)
    in_specs += [fixed(w) for w in tail]
    scratch = [pltpu.VMEM((ch, rows, wid), F32)]
    row_out = pl.BlockSpec((IB, ch, wid), lambda s, o: (row(s), 0, 0))
    out_shape, out_specs = [sds((rows, ch, wid))], [row_out]
    if split:
        out_shape += [sds((rows, ch, wid)), sds((ch, rows, wid))]
        out_specs += [row_out, pl.BlockSpec((ch, IB, wid), lambda s, o: (0, row(s), 0))]
        for first, count in split:
            out_shape.append(sds((ch, count * IB, wid)))
            out_specs.append(pl.BlockSpec((ch, IB, wid), lambda s, o, first=first, count=count: (0, jnp.clip(row(s) - first, 0, count - 1), 0)))
        scratch += [pltpu.VMEM((wid // LANES, ch * IB, LANES), F32)] * 2
    flops = 2 * rows * wid * ch * (cols + 40 * ch)
    return pl.pallas_call(
        functools.partial(pair_kernel, steps, len(a_parts), [dap] * len(b_parts), split),
        grid_spec=pltpu.PrefetchScalarGridSpec(
            num_scalar_prefetch=1, grid=(steps + row_steps,), in_specs=in_specs, out_specs=out_specs,
            scratch_shapes=scratch + scratch_b),
        out_shape=out_shape,
        compiler_params=pltpu.CompilerParams(vmem_limit_bytes=VMEM_LIMIT),
        cost_estimate=cost(flops, 4 * rows * cols * ch),
    )(order, *a_parts, *sum(b_parts, []), t_arr, u_arr, mask_f, *tail)


def attend(at, t_all, pair_loc, bias, w_q, w_kv, heads, quarter):
    num, rows, ch, wid = t_all.shape
    _, dap, _, width = pair_loc.shape
    ib = 8
    grid_spec = pltpu.PrefetchScalarGridSpec(
        num_scalar_prefetch=1,
        grid=(rows // ib,),
        in_specs=[pl.BlockSpec(memory_space=pltpu.SMEM),
                  pl.BlockSpec((num, ib, ch, wid), lambda s, r: (0, s, 0, 0)),
                  pl.BlockSpec((ib, dap, wid // dap, width), lambda s, r: (r[0] * (rows // ib) + s, 0, at, 0)),
                  pl.BlockSpec(w_q.shape, lambda s, r: (0, 0)),
                  pl.BlockSpec(w_kv.shape, lambda s, r: (0, 0))],
        out_specs=pl.BlockSpec((ib, w_q.shape[0], wid), lambda s, r: (s, 0, 0)),
    )
    return pl.pallas_call(
        lambda r_ref, *refs: attend_kernel(heads, *refs),
        grid_spec=grid_spec,
        out_shape=sds((rows, w_q.shape[0], wid)),
        cost_estimate=cost(2 * rows * wid * (num * ch * 4 * ch + width * ch), 8 * rows * wid * ch),
    )(quarter, bias, t_all, pair_loc, w_q, w_kv)


def project_out(at, where, o_parts, pair_loc, w_out, b_out, into):
    rows, dap, _, width = pair_loc.shape
    num = len(o_parts)
    sub = o_parts[0].shape[2] // dap
    ib = 16
    per_part = rows // num // ib
    z_spec = pl.BlockSpec((ib, dap, sub, width), lambda s, w: (w[s // per_part] * per_part + s % per_part, 0, at, 0))
    o_specs = [pl.BlockSpec((ib,) + o.shape[1:], lambda s, w, n=n: (jnp.clip(s - n * per_part, 0, per_part - 1), 0, 0))
               for n, o in enumerate(o_parts)]
    fixed = lambda arr: pl.BlockSpec(arr.shape, lambda s, w: (0, 0))
    extra = [] if into is None else [into]
    return pl.pallas_call(
        functools.partial(out_kernel, num, per_part),
        grid_spec=pltpu.PrefetchScalarGridSpec(
            num_scalar_prefetch=1, grid=(rows // ib,),
            in_specs=o_specs + [z_spec, fixed(w_out), fixed(b_out)] + [pl.BlockSpec(memory_space=pl.ANY)] * len(extra),
            out_specs=z_spec),
        out_shape=sds(pair_loc.shape),
        input_output_aliases={} if into is None else {num + 4: 0},
        cost_estimate=cost(4 * rows * dap * sub * width * o_parts[0].shape[1], 6 * rows * dap * sub * width),
        compiler_params=pltpu.CompilerParams(vmem_limit_bytes=OUT_VMEM),
    )(where, *o_parts, pair_loc, w_out, b_out, *extra)


def mix_weights(blk):
    ln_mix, w_mix = blk[5:7]
    ch = w_mix.shape[0]
    lnx = jnp.broadcast_to(ln_mix[:, :, None, None], (2, ch, GB, LANES))
    eye = jnp.eye(GB, dtype=BF16)
    return lnx, ((w_mix.T * 0.5)[None, :, :, None] * eye[:, None, None, :]).reshape(GB * ch, ch * GB)


def block_weights(blk, par):
    w_gate, w_up, w_down = blk[3], blk[9], blk[11]
    return mix_weights(blk) + (w_gate.T * 0.5, w_up.T, w_down.T, par)


def columns(blk, fin, next_b):
    _, _, _, _, b_gate, _, _, b_mix, ln_tr, _, b_up, _, b_down = blk
    return [b_gate * 0.5, b_mix * 0.5, b_down, *ln_tr, *fin, b_up] + ([] if next_b is None else [next_b.reshape(-1) * 0.5])


def half_w_ab(w_ab):
    return w_ab.reshape(w_ab.shape[0], -1).T * 0.5


def send(val, axes, shape, hop):
    pairs = []
    for src in range(math.prod(shape)):
        coords = []
        rest = src
        for size in reversed(shape):
            coords.insert(0, rest % size)
            rest //= size
        dst = 0
        for size, coord in zip(shape, hop(*coords)):
            dst = dst * size + coord % size
        pairs.append((src, dst))
    return lax.ppermute(val, axes, pairs)


def ring_gather(val, axes, shape, step, forward):
    first = send(val, axes, shape, functools.partial(step, 1))
    second = send(val, axes, shape, functools.partial(step, -1))
    far = send(first if forward > 0 else second, axes, shape, functools.partial(step, forward))
    return [val, first, second, far]


def side(core):
    return 1 - 2 * (core % CORES)


def solution(mesh):
    tmpl_spec = P(('batch', 'tmpl'), 'dap')
    row_spec = P(('batch', 'dap'))
    dap, tmpl = mesh.shape['dap'], mesh.shape['tmpl']
    chips = dap // CORES

    def next_chip(sign, dev):
        return (dev + sign * CORES,)

    def next_tmpl(sign, row, dev):
        return row + sign * side(dev), dev

    def gather(part, forward):
        mine = ring_gather(part, ('dap',), (dap,), next_chip, forward)
        other = [send(val, ('dap',), (dap,), lambda dev: (dev + side(dev),)) for val in mine]
        return mine + other

    def local_fn(tmpl_loc, tmpl_mask, pair_loc, mask_loc, *weights):
        _, rows, cols, ch = tmpl_loc.shape
        blk0, blk1 = (tuple(w[i] for w in weights[:BLOCK_ARGS]) for i in range(2))
        ln_fin, w_query, w_key, w_value, w_out, b_out = weights[BLOCK_ARGS:]
        heads = w_query.shape[1]
        per = cols // dap
        me = lax.axis_index('dap').astype(jnp.int32)
        chip, core = me // CORES, me % CORES
        hops = jnp.array([0, -1, 1, 2], jnp.int32)
        order = jnp.concatenate([(chip + hops) % chips * CORES + c for c in (core, CORES - 1 - core)])

        lane = jnp.arange(cols, dtype=jnp.int32)
        source = lane // UNIT % dap * per + lane // (dap * UNIT) * UNIT + lane % UNIT
        perm = (lane[:, None] == source[None, :]).astype(BF16)
        mask_f = mask_loc.astype(F32).reshape(rows, dap, per // UNIT, UNIT).swapaxes(1, 2).reshape(rows, cols)
        t_nat = tmpl_loc.reshape(rows, cols, ch).swapaxes(1, 2)
        head_par = [*blk0[0], blk0[2].reshape(-1) * 0.5]
        pars = [head_par, columns(blk0, blk1[0], blk1[2]), columns(blk1, ln_fin, None)]
        par_head = col(jnp.concatenate(pars[0]))
        par0, par1 = col(jnp.concatenate(pars[1])), col(jnp.concatenate(pars[2]))

        first_w, next_w = block_weights(blk0, par0), (half_w_ab(blk1[1]),)
        second_w = block_weights(blk1, par1)
        w_q = w_query.reshape(w_query.shape[0], -1).T
        w_kv = jnp.concatenate([w_key.reshape(ch, -1), w_value.reshape(ch, -1)], axis=1).T

        b1, into, after = [], (), ()
        for part in range(NQ):
            a1, b, u1, t1 = head(t_nat, mask_f, part, perm, par_head, half_w_ab(blk0[1]), into, after)
            into, after = (a1, u1, t1), first_w + next_w + second_w + (w_q, w_kv)
            b1.append(gather(b, 1 if part < NQ - 1 else -1))

        pieces = [(sum(PIECES[:n]), count) for n, count in enumerate(PIECES)]
        t2, u2, a2, b2 = [], [], [], []
        for q in range(NQ):
            split = [(0, rows // IB)] if q < NQ - 1 else [(first * UNIT // IB, count * UNIT // IB) for first, count in pieces]
            out = pair(q, cols // NQ, order, [a1], [b1[q]], [0], t1, u1, q, mask_f, first_w, next_w, split)
            t2.append(out[0])
            u2.append(out[1])
            a2.append(out[2])
            b2.append([gather(b, 1 if q < NQ - 1 else -1) for b in out[3:]])

        bias = MASK_BIAS * (tmpl_mask.astype(F32) - 1.0)
        z_view = pair_loc.reshape(rows, dap, per, pair_loc.shape[2])
        quarter = lax.axis_index('tmpl').astype(jnp.int32).reshape(1)
        where = (quarter + side(core) * hops) % tmpl
        z_out = None
        for n, (first, count) in enumerate(pieces):
            wid = count * UNIT * dap
            b_parts = [b2[k][0] for k in range(NQ - 1)] + [b2[NQ - 1][n]]
            q, at = first * UNIT * dap * NQ // cols, first // count
            t_index = at % (cols // NQ // wid)
            fin, = pair(at, wid, order, a2, b_parts, [at] * (NQ - 1) + [0], t2[q], u2[q], t_index, mask_f,
                        second_w, (), ())
            fin = fin.reshape(tmpl, rows // tmpl, ch, wid)
            t_all = lax.all_to_all(fin, 'tmpl', 0, 0)
            o_loc = attend(at, t_all, z_view, bias, w_q, w_kv, heads, quarter)
            o_parts = ring_gather(o_loc, ('tmpl', 'dap'), (tmpl, dap), next_tmpl, 1)
            z_out = project_out(at, where, o_parts, z_view, w_out.reshape(-1, w_out.shape[2]), b_out[None], z_out)
        return z_out.reshape(pair_loc.shape)

    in_specs = (tmpl_spec, P('batch'), row_spec, row_spec) + (P(),) * (BLOCK_ARGS + 6)
    return jax.shard_map(local_fn, mesh=mesh, in_specs=in_specs, out_specs=row_spec, check_vma=False)
```
